256 devices in a mesh: group: 2 (over z), tp: 16 (over x, core), dp: 8 (over y).
Axes of the slice: x: 8, y: 8, z: 2, core: 2. Of those that a mesh axis runs over, the one named last changes fastest.
The devices are a block of a 8x8x16 slice.
Arguments:
- patches: bfloat16 [1024, 128, 1280], P(('group', 'tp', 'dp')), parts along dimension 0, may hold values from -38 to 38, as said below
- patch_counts: int32 [1024], P(('group', 'tp', 'dp')), parts along dimension 0, may hold values from 0 to 128, as said below
- encoder_index: int32 [1024], P(('group', 'tp', 'dp')), parts along dimension 0, may hold values from 0 to 7, as said below
- vit_gain: float32 [1280], replicated, may hold values from 0.1 to 1.9
- vit_up: bfloat16 [1280, 5120], P(None, 'tp'), may hold values from -0.15625 to 0.15625
- vit_down: bfloat16 [5120, 1280], P('tp'), may hold values from -0.078125 to 0.078125
- queries: bfloat16 [64, 32, 128], P(('group', 'dp')), parts along dimension 0, may hold values from -20 to 20
- cache_keys: bfloat16 [64, 4, 8192, 128], P(('group', 'dp'), None, 'tp'), parts along dimension 0, may hold values from -6 to 6
- cache_values: bfloat16 [64, 4, 8192, 128], P(('group', 'dp'), None, 'tp'), parts along dimension 0, may hold values from -6 to 6
- new_keys: bfloat16 [64, 4, 128], P(('group', 'dp')), parts along dimension 0, may hold values from -6 to 6
- new_values: bfloat16 [64, 4, 128], P(('group', 'dp')), parts along dimension 0, may hold values from -6 to 6
- kv_lengths: int32 [64], P(('group', 'dp')), parts along dimension 0, may hold values from 2 to 8192, as said below
- out_weight: bfloat16 [4096, 8192], P(None, 'tp'), may hold values from -0.09375 to 0.09375
Outputs:
- embeddings: bfloat16 [768, 128, 1280], P(('group', 'tp', 'dp')), parts along dimension 0
- decoded: bfloat16 [64, 8192], P(('group', 'dp'), 'tp'), parts along dimension 0
The draws below stay inside these ranges and needn't reach their ends.
There are 2 independent parts, one for each index of `group`. The reference program is written for one: setup_inputs(seed, part) draws one part's arguments, and reference() takes and returns one part's arrays. A program takes and returns all parts, laid end to end along the dimension named above; an argument that names none is the same for every part. Nothing has to cross between parts.
Inputs may be any that keep to these rules, and one draw needn't show every extreme that they name: `patches`: draws of spread scale. `patch_counts`: 0 marks an empty slot. Each device holds between 1 and 4 non-empty slots and some device holds 4; each tp row of 8 devices holds exactly 24 non-empty slots; some slot has 128 patches. `encoder_index`: indices into the dp axis within the slot's own tp row. The non-empty slots of one device name distinct encoders, and every encoder is named by exactly 3 non-empty slots of its tp row. Entries of empty slots carry no meaning. `kv_lengths`: some sequence uses all 8192 positions.
All inputs are finite; a program needn't handle non-finite values.
Results may differ from the reference program's by a relative error of at most 0.015.
Values may be sent and summed in bfloat16 or wider, within the bound.
A program may use at most 192 MiB of HBM per device.

```python
import jax
import jax.numpy as jnp
from jax import lax

VD = 1280
VF = 5120
PATCH = 128
IMG_MAX = 4
RECV_MAX = 3
DM = 8192
HEADS = 32
KVH = 4
HD = 128
CTX = 8192
SRC_SLOTS = 512
BATCH = 32
N_TP = 16
N_DP = 8


def image_plan(key):
    base = jax.random.fold_in(key, 5)
    key_rank, key_order, key_target, key_count = jax.random.split(base, 4)
    ranking = jax.vmap(lambda item: jax.random.permutation(item, N_DP))(jax.random.split(key_rank, N_TP))
    quarter = N_DP // 4
    live_count = jnp.where(ranking < 2 * quarter, IMG_MAX, jnp.where(ranking < 3 * quarter, 3, 1))
    ordering = jax.vmap(lambda item: jax.random.permutation(item, IMG_MAX))(jax.random.split(key_order, N_TP * N_DP))
    ordering = ordering.reshape(N_TP, N_DP, IMG_MAX)
    live_slot = ordering < live_count[:, :, None]
    offsets = jnp.cumsum(live_count, axis=1) - live_count
    position = (offsets[:, :, None] + ordering) % N_DP
    targets = jax.vmap(lambda item: jax.random.permutation(item, N_DP))(jax.random.split(key_target, N_TP))
    chosen = jnp.take_along_axis(targets, position.reshape(N_TP, N_DP * IMG_MAX), axis=1).reshape(N_TP, N_DP, IMG_MAX)
    own_index = jnp.broadcast_to(jnp.arange(N_DP, dtype=jnp.int32)[None, :, None], chosen.shape)
    encoder_index = jnp.where(live_slot, chosen, own_index)
    counts = jax.random.randint(key_count, (N_TP, N_DP, IMG_MAX), 1, PATCH + 1)
    full_slot = live_slot & (ordering == 0) & (live_count == IMG_MAX)[:, :, None]
    counts = jnp.where(full_slot, PATCH, counts)
    counts = jnp.where(live_slot, counts, 0)
    return (counts.reshape(-1).astype(jnp.int32), encoder_index.reshape(-1).astype(jnp.int32))


def draw_patch_counts(key, part):
    return image_plan(key)[0]


def draw_encoder_index(key, part):
    return image_plan(key)[1]


def draw_patches(key, part):
    key_base, key_rows, key_cols = jax.random.split(jax.random.fold_in(key, 9), 3)
    shape = (SRC_SLOTS, PATCH, VD)
    row_scale = jnp.exp(jax.random.uniform(key_rows, (SRC_SLOTS, PATCH, 1), minval=-1.05, maxval=1.25))
    col_scale = jnp.exp(jax.random.uniform(key_cols, (1, 1, VD), minval=-0.5, maxval=0.58))
    values = jnp.clip(jax.random.normal(key_base, shape), -6.0, 6.0)
    return (values * row_scale * col_scale).astype(jnp.bfloat16)


def draw_queries(key, part):
    key_base = jax.random.fold_in(key, 23)
    shape = (BATCH, HEADS, HD)
    values = jnp.clip(jax.random.normal(key_base, shape), -6.0, 6.0)
    return values.astype(jnp.bfloat16)


def draw_cache_keys(key, part):
    key_base = jax.random.fold_in(key, 29)
    shape = (BATCH, KVH, CTX, HD)
    values = jnp.clip(jax.random.normal(key_base, shape), -6.0, 6.0)
    return values.astype(jnp.bfloat16)


def draw_kv_lengths(key, part):
    key_length, key_full = jax.random.split(jax.random.fold_in(key, 31), 2)
    lengths = jax.random.randint(key_length, (BATCH,), 2, CTX + 1)
    chosen = jax.random.randint(key_full, (), 0, BATCH)
    lengths = jnp.where(jnp.arange(BATCH) == chosen, CTX, lengths)
    return lengths.astype(jnp.int32)


def shard_levels(stream_key, dims, cuts, low, high):
    level, own = 1.0, jax.random.fold_in(stream_key, 6)
    for dim, blocks in cuts:
        heights = jnp.exp(jax.random.uniform(jax.random.fold_in(own, dim), (blocks,), jnp.float32, low / len(cuts), high / len(cuts)))
        level = level * jnp.repeat(heights, dims[dim] // blocks).reshape([-1 if axis == dim else 1 for axis in range(len(dims))])
    return level


def bell_draw(own_key, extent, scale, reach, cuts=(), kind=jnp.bfloat16):
    level = shard_levels(own_key, extent, cuts, -0.22, 0.18) if cuts else 1.0
    entries = jax.random.normal(own_key, extent, jnp.float32) * scale * level
    return jnp.minimum(jnp.maximum(entries, -reach), reach).astype(kind)


def setup_inputs(seed: int = 0, part: int = 0) -> dict:
    arg_keys = jax.random.split(jax.random.key(seed), 14)
    own_keys = jax.random.split(jax.random.fold_in(arg_keys[13], part), 14)
    patches = draw_patches(jax.random.fold_in(jax.random.fold_in(arg_keys[13], part), 71), part)
    patch_counts = draw_patch_counts(jax.random.fold_in(jax.random.fold_in(arg_keys[13], part), 71), part)
    encoder_index = draw_encoder_index(jax.random.fold_in(jax.random.fold_in(arg_keys[13], part), 71), part)
    vit_gain = jnp.clip(1.0 + 0.18 * jax.random.normal(arg_keys[3], (VD,), jnp.float32), 0.1, 1.9)
    vit_up = bell_draw(arg_keys[4], (VD, VF), VD ** -0.5, 0.15625, ((1, 16),))
    vit_down = bell_draw(arg_keys[5], (VF, VD), VF ** -0.5, 0.078125, ((0, 16),))
    queries = draw_queries(jax.random.fold_in(jax.random.fold_in(arg_keys[13], part), 71), part)
    cache_keys = draw_cache_keys(jax.random.fold_in(jax.random.fold_in(arg_keys[13], part), 71), part)
    cache_values = bell_draw(own_keys[8], (BATCH, KVH, CTX, HD), 1.0, 6.0, ((0, 8), (2, 16)))
    new_keys = bell_draw(own_keys[9], (BATCH, KVH, HD), 1.0, 6.0, ((0, 8),))
    new_values = bell_draw(own_keys[10], (BATCH, KVH, HD), 1.0, 6.0, ((0, 8),))
    kv_lengths = draw_kv_lengths(jax.random.fold_in(jax.random.fold_in(arg_keys[13], part), 71), part)
    out_weight = bell_draw(arg_keys[12], (HEADS * HD, DM), (HEADS * HD) ** -0.5, 0.09375, ((1, 16),))
    return dict(patches=patches, patch_counts=patch_counts, encoder_index=encoder_index, vit_gain=vit_gain, vit_up=vit_up, vit_down=vit_down, queries=queries, cache_keys=cache_keys, cache_values=cache_values, new_keys=new_keys, new_values=new_values, kv_lengths=kv_lengths, out_weight=out_weight)


def quick_gelu(values):
    return values * jax.nn.sigmoid(1.702 * values)

def encode_rows(block_rows, vit_gain, vit_up, vit_down):
    xfloat = block_rows.astype(jnp.float32)
    center = xfloat - lax.optimization_barrier(jnp.mean(xfloat, axis=-1, keepdims=True))
    spread = lax.optimization_barrier(jnp.mean(center * center, axis=-1, keepdims=True))
    normed = (center * lax.rsqrt(spread + 1e-06) * vit_gain).astype(jnp.bfloat16)
    hidden = quick_gelu(jnp.dot(normed, vit_up, preferred_element_type=jnp.float32)).astype(jnp.bfloat16)
    return (xfloat + jnp.dot(hidden, vit_down, preferred_element_type=jnp.float32)).astype(jnp.bfloat16)

def reference(patches, patch_counts, encoder_index, vit_gain, vit_up, vit_down, queries, cache_keys, cache_values, new_keys, new_values, kv_lengths, out_weight):
    row_slots = N_DP * IMG_MAX
    counts_rows = patch_counts.reshape(N_TP, row_slots)
    targets_rows = encoder_index.reshape(N_TP, row_slots)
    member = (counts_rows > 0)[:, None, :] & (targets_rows[:, None, :] == jnp.arange(N_DP, dtype=jnp.int32)[None, :, None])
    ranking = (jnp.cumsum(member.astype(jnp.int32), axis=2) - 1).astype(jnp.int32)
    hits = member[:, :, None, :] & (ranking[:, :, None, :] == jnp.arange(RECV_MAX, dtype=jnp.int32)[None, None, :, None])
    flat_index = jnp.arange(row_slots, dtype=jnp.int32)
    source = lax.optimization_barrier(jnp.sum(jnp.where(hits, flat_index, 0), axis=-1)).astype(jnp.int32)
    source = (source + (jnp.arange(N_TP, dtype=jnp.int32) * row_slots)[:, None, None]).astype(jnp.int32)
    kept = lax.optimization_barrier(jnp.sum(jnp.where(hits, counts_rows[:, None, None, :], 0), axis=-1)).astype(jnp.int32)

    def one_block(item):
        index, count = item
        block = lax.dynamic_index_in_dim(patches, index, 0, keepdims=False)
        encoded = encode_rows(block, vit_gain, vit_up, vit_down)
        keep = jnp.arange(PATCH, dtype=jnp.int32) < count
        return jnp.where(keep[:, None], encoded, jnp.zeros_like(encoded))
    embeddings = lax.map(one_block, (source.reshape(-1).astype(jnp.int32), kept.reshape(-1).astype(jnp.int32)))
    scale = HD ** (-0.5)

    def attend_one(item):
        query, keys_seq, values_seq, key_new, value_new, length = item
        grouped = query.astype(jnp.float32).reshape(KVH, HEADS // KVH, HD)
        scores = jnp.einsum('kgd,kpd->kgp', grouped, keys_seq.astype(jnp.float32)) * scale
        valid = jnp.arange(CTX, dtype=jnp.int32) < length
        scores = jnp.where(valid[None, None, :], scores, -1e+30)
        own = jnp.einsum('kgd,kd->kg', grouped, key_new.astype(jnp.float32)) * scale
        top = jnp.maximum(lax.optimization_barrier(jnp.max(scores, axis=-1)), own)
        weights = jnp.exp(scores - top[..., None])
        own_weight = jnp.exp(own - top)
        total = lax.optimization_barrier(jnp.sum(weights, axis=-1)) + own_weight
        rounded = lax.optimization_barrier(weights.astype(jnp.bfloat16)).astype(jnp.float32)
        own_rounded = lax.optimization_barrier(own_weight.astype(jnp.bfloat16)).astype(jnp.float32)
        mixed = jnp.einsum('kgp,kpd->kgd', rounded, values_seq.astype(jnp.float32))
        mixed = mixed + own_rounded[..., None] * value_new.astype(jnp.float32)[:, None, :]
        return (mixed / total[..., None]).reshape(HEADS * HD).astype(jnp.bfloat16)
    attended = lax.map(attend_one, (queries, cache_keys, cache_values, new_keys, new_values, kv_lengths))
    decoded = jnp.dot(attended, out_weight, preferred_element_type=jnp.float32).astype(jnp.bfloat16)
    return (embeddings, decoded)
```

```python
import functools

import jax
import jax.numpy as jnp
from jax import lax
from jax.experimental import pallas as pl
from jax.experimental.pallas import tpu as pltpu
from jax.sharding import PartitionSpec as P

MESH = pl.DeviceIdType.MESH
RECV_MAX = 3
CORES = 2
F32 = jnp.float32
BF16 = jnp.bfloat16


def rcopy(src, dst, send, recv, **where):
    return pltpu.make_async_remote_copy(
        src_ref=src,
        dst_ref=dst,
        send_sem=send,
        recv_sem=recv,
        device_id=where,
        device_id_type=MESH,
    )


def drain(ref, sem):
    pltpu.make_async_copy(ref, ref, sem).wait()


def kernel(
    sizes,
    counts,
    enc,
    lens,
    patches,
    gain,
    up,
    down,
    q,
    keys,
    values,
    nk,
    nv,
    ow,
    emb,
    dec,
    w,
    upv,
    pv,
    outgoing,
    arrived,
    kv,
    vv,
    owv,
    meta_out,
    meta_in,
    meta_s,
    rs_src,
    rs_dst,
    ag_dst,
    own_buf,
    nv_buf,
    normed,
    acc,
    local_sem,
    x_recv,
    z_recv,
    d_recv,
    x_send,
    z_send,
    d_send,
    da_send,
    dz_send,
    a_sem,
    m_sem,
    rs_sem,
    ag_sem,
):
    n_tp, n_dp, paired = sizes
    ring = n_tp // CORES
    hops = ring - 1
    half = w.shape[3]
    zrows = (half * 3 // 10) // 16 * 16 if paired else 0
    xrows = half - zrows
    t = lax.axis_index("tp")
    y = lax.axis_index("dp")
    g = lax.axis_index("group")
    par = lax.rem(g, 2)
    right = lax.rem(t + CORES, n_tp)
    left = lax.rem(t + n_tp - CORES, n_tp)
    sib = t + 1 - 2 * lax.rem(t, 2)
    peer = g + 1 - 2 * par
    xstart = pl.multiple_of(par * zrows, 16)
    zstart = pl.multiple_of(par * xrows, 16)
    zother = pl.multiple_of((1 - par) * xrows, 16)
    slots = patches.shape[0]

    barrier = pltpu.get_barrier_semaphore()
    for d in range(1, n_tp):
        pl.semaphore_signal(
            barrier, inc=1, device_id={"tp": lax.rem(t + d, n_tp)}, device_id_type=MESH
        )
    for d in range(1, n_dp):
        pl.semaphore_signal(
            barrier, inc=1, device_id={"dp": lax.rem(y + d, n_dp)}, device_id_type=MESH
        )
    if paired:
        pl.semaphore_signal(barrier, inc=1, device_id={"group": peer}, device_id_type=MESH)

    loads = [
        pltpu.make_async_copy(up, upv, local_sem.at[0]),
        pltpu.make_async_copy(down.at[pl.ds(0, half)], w.at[1, 0, 0], local_sem.at[1]),
        pltpu.make_async_copy(down.at[pl.ds(half, half)], w.at[1, 0, 1], local_sem.at[2]),
        pltpu.make_async_copy(patches, pv, local_sem.at[3]),
        pltpu.make_async_copy(keys, kv, local_sem.at[4]),
        pltpu.make_async_copy(values, vv, local_sem.at[5]),
        pltpu.make_async_copy(ow, owv, local_sem.at[6]),
    ]
    for load in loads:
        load.start()

    row = lax.broadcasted_iota(jnp.int32, (8, 128), 0)
    lane = lax.broadcasted_iota(jnp.int32, (8, 128), 1)
    meta = jnp.zeros((8, 128), jnp.int32)
    for s in range(slots):
        meta = jnp.where((row == 0) & (lane == s), counts[s], meta)
        meta = jnp.where((row == 1) & (lane == s), enc[s], meta)
    meta_out[...] = meta
    meta_in[y] = meta

    loads[0].wait()
    w[0, 0, 0:2] = jnp.transpose(upv[...].astype(F32)).astype(BF16).reshape(2, half, upv.shape[0])

    pl.semaphore_wait(barrier, n_tp - 1 + n_dp - 1 + (1 if paired else 0))

    def x_copy(lane_, d, r):
        rows = pl.ds(xstart, xrows)
        return rcopy(
            w.at[lane_, r, d, rows],
            w.at[lane_, r + 1, d, rows],
            x_send,
            x_recv.at[lane_, d, r],
            tp=right if d == 0 else left,
        )

    def z_copy(lane_, d, r):
        rows = pl.ds(zstart, zrows)
        return rcopy(
            w.at[lane_, r, d, rows],
            w.at[lane_, r, d, rows],
            z_send,
            z_recv.at[lane_, d, r],
            group=peer,
        )

    def d_copy(lane_, d, r, part):
        rows, send = {
            0: (pl.ds(xstart, xrows), d_send),
            1: (pl.ds(zother, zrows), dz_send),
            2: (pl.ds(0, half), da_send),
        }[part]
        return rcopy(
            w.at[lane_, r, d, rows],
            w.at[lane_, r, 2 + d, rows],
            send,
            d_recv.at[lane_, d, r, min(part, 1) if part < 2 else 0],
            tp=sib,
        )

    loads[1].wait()
    loads[2].wait()
    for lane_ in (1, 0):
        for d in (0, 1):
            x_copy(lane_, d, 0).start()

    loads[3].wait()

    def stage(e, carry):
        slot = jnp.int32(0)
        for s in range(slots):
            slot = slot + jnp.where((counts[s] > 0) & (enc[s] == e), s, 0)
        outgoing[e] = pv[slot]
        return carry

    lax.fori_loop(0, n_dp, stage, 0)
    for d in range(1, n_dp):
        to = lax.rem(y + d, n_dp)
        rcopy(meta_out, meta_in.at[y], m_sem.at[0], m_sem.at[1], dp=to).start()
    far_first = sorted(range(1, n_dp), key=lambda d: -min(d, n_dp - d))
    for d in far_first:
        to = lax.rem(y + d, n_dp)
        rcopy(outgoing.at[to], arrived.at[y], a_sem.at[0], a_sem.at[1], dp=to).start()
    arrived[y] = outgoing[y]
    for lane_ in (1, 0):
        for d in (0, 1):
            d_copy(lane_, d, 0, 2).start()

    seqs, kvh, span, hd = kv.shape
    per = q.shape[1] // kvh
    scale = hd**-0.5
    own_heads = (kvh * per) // n_tp

    def attend_local():
        loads[4].wait()
        loads[5].wait()
        wide = lax.broadcasted_iota(jnp.int32, (per, 128), 1)
        for s in range(seqs):
            pos = t * span + lax.broadcasted_iota(jnp.int32, (per, span), 1)
            valid = pos < lens[s]
            for h in range(kvh):
                query = q[s, h * per : (h + 1) * per, :]
                scores = (
                    lax.dot_general(
                        query, kv[s, h], (((1,), (1,)), ((), ())), preferred_element_type=F32
                    )
                    * scale
                )
                scores = jnp.where(valid, scores, -1e30)
                own = (
                    jnp.sum(
                        query.astype(F32) * nk[s, h : h + 1, :].astype(F32), axis=1, keepdims=True
                    )
                    * scale
                )
                top = jnp.maximum(jnp.max(scores, axis=1, keepdims=True), own)
                weights = jnp.exp(scores - top)
                total = jnp.sum(weights, axis=1, keepdims=True)
                mix = jnp.dot(weights.astype(BF16), vv[s, h], preferred_element_type=F32)
                stats = jnp.where(wide < 64, top, total)
                ownw = jnp.broadcast_to(own, (per, 128))
                fresh = nv[s, h : h + 1, :].astype(F32)
                for i in range(per):
                    head = h * per + i
                    p, j = head // own_heads, head % own_heads
                    at = seqs * j + s
                    rs_src[p, at : at + 1, :] = mix[i : i + 1, :]
                    rs_src[p, 8 + at : 9 + at, :] = stats[i : i + 1, :]
                    own_buf[p, at : at + 1, :] = ownw[i : i + 1, :]
                    nv_buf[p, at : at + 1, :] = fresh
        rs_dst[t] = rs_src[t]
        for d in range(1, n_tp):
            to = lax.rem(t + d, n_tp)
            rcopy(rs_src.at[to], rs_dst.at[t], rs_sem.at[0], rs_sem.at[1], tp=to).start()

    def attend_merge():
        some = pl.ds(0, n_tp - 1)
        drain(rs_dst.at[some], rs_sem.at[1])
        own = own_buf[t][:, 0:1]
        tops = [rs_dst[p, 8:16, 0:1] for p in range(n_tp)]
        top = own
        for m in tops:
            top = jnp.maximum(top, m)
        own_weight = jnp.exp(own - top)
        total = own_weight
        mixed = own_weight.astype(BF16).astype(F32) * nv_buf[t]
        for p in range(n_tp):
            factor = jnp.exp(tops[p] - top)
            total = total + rs_dst[p, 8:16, 64:65] * factor
            mixed = mixed + rs_dst[p, 0:8, :] * factor
        ag_dst[t] = (mixed / total).astype(BF16).astype(F32)
        for d in range(1, n_tp):
            to = lax.rem(t + d, n_tp)
            rcopy(ag_dst.at[t], ag_dst.at[t], ag_sem.at[0], ag_sem.at[1], tp=to).start()

    def project():
        loads[6].wait()
        drain(ag_dst.at[pl.ds(0, n_tp - 1)], ag_sem.at[1])
        wide = own_heads * hd
        total = jnp.zeros((8, owv.shape[1]), F32)
        which = lax.broadcasted_iota(jnp.int32, (8, hd), 0) // seqs
        for p in range(n_tp):
            block = ag_dst[p]
            lhs = jnp.concatenate(
                [jnp.where(which == j, block, 0.0) for j in range(own_heads)], axis=1
            ).astype(BF16)
            total = total + jnp.dot(
                lhs, owv[p * wide : (p + 1) * wide, :], preferred_element_type=F32
            )
        out = total[0:seqs]
        for j in range(1, own_heads):
            out = out + total[j * seqs : (j + 1) * seqs]
        dec[...] = out.astype(BF16)

    kept = []

    def images():
        drain(meta_in.at[pl.ds(0, n_dp - 1)], m_sem.at[1])
        small = pltpu.make_async_copy(meta_in, meta_s, local_sem.at[7])
        small.start()
        small.wait()
        drain(arrived.at[pl.ds(0, n_dp - 1)], a_sem.at[1])
        found = jnp.int32(0)
        pick = [jnp.int32(0)] * RECV_MAX
        keep = [jnp.int32(0)] * RECV_MAX
        for src in range(n_dp):
            count = jnp.int32(0)
            for s in range(slots):
                c = meta_s[src, 0, s]
                count = count + jnp.where((c > 0) & (meta_s[src, 1, s] == y), c, 0)
            for k in range(RECV_MAX):
                hit = (count > 0) & (found == k)
                pick[k] = jnp.where(hit, src, pick[k])
                keep[k] = jnp.where(hit, count, keep[k])
            found = found + jnp.where(count > 0, 1, 0)
        kept.extend(keep)
        rows = arrived.shape[1]
        for k in range(RECV_MAX):
            x = arrived[pick[k]].astype(F32)
            acc[k * rows : (k + 1) * rows, :] = x
            center = x - jnp.mean(x, axis=1, keepdims=True)
            spread = jnp.mean(center * center, axis=1, keepdims=True)
            n = (center * lax.rsqrt(spread + 1e-06) * gain[...]).astype(BF16)
            normed[k * rows : (k + 1) * rows, :] = n

    def vit(r):
        width = w.shape[4]
        a = w[0, r].reshape(4 * half, width)
        pre = lax.dot_general(
            normed[...], a, (((1,), (1,)), ((), ())), preferred_element_type=F32
        )
        hidden = (pre * jax.nn.sigmoid(1.702 * pre)).astype(BF16)
        b = w[1, r].reshape(4 * half, width)
        acc[...] += jnp.dot(hidden, b, preferred_element_type=F32)

    def vit_range(lo, hi):
        def body(r, carry):
            vit(r)
            return carry

        lax.fori_loop(lo, hi, body, 0)

    def finish(r):
        if paired:
            for lane_ in (1, 0):
                for d in (0, 1):
                    drain(w.at[lane_, r, d, pl.ds(zother, zrows)], z_recv.at[lane_, d, r])
                    d_copy(lane_, d, r, 1).start()

    def ready(r):
        for lane_ in (1, 0):
            for d in (0, 1):
                if r == 0:
                    drain(w.at[lane_, r, 2 + d], d_recv.at[lane_, d, r, 0])
                else:
                    drain(w.at[lane_, r, 2 + d, pl.ds(xstart, xrows)], d_recv.at[lane_, d, r, 0])
                    if paired:
                        drain(
                            w.at[lane_, r, 2 + d, pl.ds(zother, zrows)], d_recv.at[lane_, d, r, 1]
                        )

    work = {1: attend_local, 2: attend_merge, 3: project}
    first_vit = max(hops - 2, 4)
    for r in range(1, hops + 1):
        for lane_ in (1, 0):
            for d in (0, 1):
                rows = pl.ds(xstart, xrows)
                drain(w.at[lane_, r, d, rows], x_recv.at[lane_, d, r - 1])
                if r < hops:
                    x_copy(lane_, d, r).start()
                if paired:
                    z_copy(lane_, d, r).start()
                d_copy(lane_, d, r, 0).start()
        if r > 1:
            finish(r - 1)
        if r in work:
            work[r]()
        if r == first_vit:
            images()
            ready(0)
            for i in range(1, r - 1):
                ready(i)
            vit_range(0, r - 1)
        elif r > first_vit:
            ready(r - 2)
            vit_range(r - 2, r - 1)
    finish(hops)
    ready(hops - 1)
    vit_range(hops - 1, hops)
    ready(hops)
    vit_range(hops, hops + 1)

    rows = arrived.shape[1]
    for k in range(RECV_MAX):
        at = lax.broadcasted_iota(jnp.int32, (rows, acc.shape[1]), 0)
        block = acc[k * rows : (k + 1) * rows, :]
        emb[k] = jnp.where(at < kept[k], block, 0.0).astype(BF16)

    drain(w.at[:, pl.ds(0, hops), pl.ds(0, 2), pl.ds(0, xrows)], x_send)
    drain(w.at[:, pl.ds(0, hops), pl.ds(0, 2), pl.ds(0, xrows)], d_send)
    drain(w.at[:, pl.ds(0, 1), pl.ds(0, 2)], da_send)
    if paired:
        drain(w.at[:, pl.ds(0, hops), pl.ds(0, 2), pl.ds(0, zrows)], z_send)
        drain(w.at[:, pl.ds(0, hops), pl.ds(0, 2), pl.ds(0, zrows)], dz_send)
    drain(outgoing.at[pl.ds(0, n_dp - 1)], a_sem.at[0])
    drain(meta_in.at[pl.ds(0, n_dp - 1)], m_sem.at[0])
    drain(rs_src.at[pl.ds(0, n_tp - 1)], rs_sem.at[0])
    drain(ag_dst.at[pl.ds(0, n_tp - 1)], ag_sem.at[0])


def local(sizes, *args):
    (
        patches,
        patch_counts,
        encoder_index,
        vit_gain,
        vit_up,
        vit_down,
        queries,
        cache_keys,
        cache_values,
        new_keys,
        new_values,
        kv_lengths,
        out_weight,
    ) = args
    n_tp, n_dp, paired = sizes
    slots, rows, width = patches.shape
    units = vit_down.shape[0]
    half = units // 2
    ring = n_tp // CORES
    seqs = queries.shape[0]
    columns = out_weight.shape[1]
    smem = pl.BlockSpec(memory_space=pltpu.SMEM)
    vmem = pl.BlockSpec(memory_space=pltpu.VMEM)
    hbm = pl.BlockSpec(memory_space=pl.ANY)
    dma = pltpu.SemaphoreType.DMA
    return pl.pallas_call(
        functools.partial(kernel, sizes),
        out_shape=(
            jax.ShapeDtypeStruct((RECV_MAX, rows, width), BF16),
            jax.ShapeDtypeStruct((seqs, columns), BF16),
        ),
        in_specs=[smem, smem, smem, hbm, vmem, hbm, hbm, vmem, hbm, hbm, vmem, vmem, hbm],
        out_specs=(vmem, vmem),
        scratch_shapes=[
            pltpu.VMEM((2, ring, 4, half, width), BF16),
            pltpu.VMEM(vit_up.shape, BF16),
            pltpu.VMEM(patches.shape, BF16),
            pltpu.VMEM((n_dp, rows, width), BF16),
            pltpu.VMEM((n_dp, rows, width), BF16),
            pltpu.VMEM(cache_keys.shape, BF16),
            pltpu.VMEM(cache_values.shape, BF16),
            pltpu.VMEM(out_weight.shape, BF16),
            pltpu.VMEM((8, 128), jnp.int32),
            pltpu.VMEM((n_dp, 8, 128), jnp.int32),
            pltpu.SMEM((n_dp, 8, 128), jnp.int32),
            pltpu.VMEM((n_tp, 16, 128), F32),
            pltpu.VMEM((n_tp, 16, 128), F32),
            pltpu.VMEM((n_tp, 8, 128), F32),
            pltpu.VMEM((n_tp, 8, 128), F32),
            pltpu.VMEM((n_tp, 8, 128), F32),
            pltpu.VMEM((RECV_MAX * rows, width), BF16),
            pltpu.VMEM((RECV_MAX * rows, width), F32),
            dma((8,)),
            dma((2, 2, ring - 1)),
            dma((2, 2, ring)),
            dma((2, 2, ring, 2)),
            dma,
            dma,
            dma,
            dma,
            dma,
            dma((2,)),
            dma((2,)),
            dma((2,)),
            dma((2,)),
        ],
        compiler_params=pltpu.CompilerParams(
            collective_id=0, has_side_effects=True, vmem_limit_bytes=62 * 1024 * 1024
        ),
        name="step",
    )(
        patch_counts,
        encoder_index,
        kv_lengths,
        patches,
        vit_gain.reshape(1, width),
        vit_up,
        vit_down,
        queries,
        cache_keys,
        cache_values,
        new_keys,
        new_values,
        out_weight,
    )


def solution(mesh):
    groups = mesh.shape["group"]
    sizes = (mesh.shape["tp"], mesh.shape["dp"], groups % 2 == 0)
    return jax.shard_map(
        functools.partial(local, sizes),
        mesh=mesh,
        in_specs=(
            P(("group", "tp", "dp"), None, None),
            P(("group", "tp", "dp")),
            P(("group", "tp", "dp")),
            P(),
            P(None, "tp"),
            P("tp", None),
            P(("group", "dp"), None, None),
            P(("group", "dp"), None, "tp", None),
            P(("group", "dp"), None, "tp", None),
            P(("group", "dp"), None, None),
            P(("group", "dp"), None, None),
            P(("group", "dp")),
            P(None, "tp"),
        ),
        out_specs=(P(("group", "tp", "dp"), None, None), P(("group", "dp"), "tp")),
        check_vma=False,
    )
```

```python
import functools

import jax
import jax.numpy as jnp
from jax import lax
from jax.experimental import pallas as pl
from jax.experimental.pallas import tpu as pltpu
from jax.sharding import PartitionSpec as P

MESH = pl.DeviceIdType.MESH
RECV_MAX = 3
CORES = 2
PARTS = 2
F32 = jnp.float32
BF16 = jnp.bfloat16


def rcopy(src, dst, send, recv, **where):
    return pltpu.make_async_remote_copy(
        src_ref=src,
        dst_ref=dst,
        send_sem=send,
        recv_sem=recv,
        device_id=where,
        device_id_type=MESH,
    )


def drain(ref, sem):
    pltpu.make_async_copy(ref, ref, sem).wait()


def split_rows(half):
    tiles = half // 16
    zrows, yrows = tiles * 3 // 10 * 16, tiles // 10 * 16
    return zrows, yrows, half - 2 * zrows - 2 * yrows


def kernel(
    sizes,
    counts,
    enc,
    lens,
    patches,
    gain,
    up,
    down,
    q,
    keys,
    values,
    nk,
    nv,
    ow,
    emb,
    dec,
    w,
    pv,
    outgoing,
    arrived_a,
    arrived_b,
    kv,
    vv,
    owv,
    meta_out,
    meta_in,
    meta_s,
    rs_src,
    rs_dst,
    ag_dst,
    own_buf,
    nv_buf,
    normed,
    turned,
    acc,
    part_out,
    part_in,
    local_sem,
    x_recv,
    z_recv,
    y_recv,
    x_send,
    z_send,
    y_send,
    a_send,
    a_recv,
    m_sem,
    rs_sem,
    ag_sem,
    tok_send,
    tok_recv,
    part_send,
    part_recv,
):
    n_tp, n_dp = sizes
    ring = n_tp // CORES
    hops = ring - 1
    half = w.shape[3]
    zrows, yrows, drows = split_rows(half)
    t = lax.axis_index("tp")
    y = lax.axis_index("dp")
    g = lax.axis_index("group")
    gpar = lax.rem(g, 2)
    ypar = lax.rem(y, 2)
    core = lax.rem(t, CORES)
    right = lax.rem(t + CORES, n_tp)
    left = lax.rem(t + n_tp - CORES, n_tp)
    sib = t + 1 - 2 * core
    peer = g + 1 - 2 * gpar
    above, below = lax.rem(y + 1, n_dp), lax.rem(y + n_dp - 1, n_dp)
    zmine = pl.multiple_of(gpar * (half - zrows), 16)
    zother = pl.multiple_of((1 - gpar) * (half - zrows), 16)
    ymine = pl.multiple_of(zrows + ypar * (yrows + drows), 16)
    yother = pl.multiple_of(zrows + (1 - ypar) * (yrows + drows), 16)
    lanes = ((zmine, zrows), (ymine, yrows), (zrows + yrows, drows))
    slots, rows, width = patches.shape
    few = rows // PARTS
    arrived = (arrived_a, arrived_b)

    barrier = pltpu.get_barrier_semaphore()
    for d in range(1, n_tp):
        pl.semaphore_signal(
            barrier, inc=1, device_id={"tp": lax.rem(t + d, n_tp)}, device_id_type=MESH
        )
    for d in range(1, n_dp):
        pl.semaphore_signal(
            barrier, inc=1, device_id={"dp": lax.rem(y + d, n_dp)}, device_id_type=MESH
        )
    pl.semaphore_signal(barrier, inc=1, device_id={"group": peer}, device_id_type=MESH)

    loads = [
        pltpu.make_async_copy(up.at[pl.ds(0, half)], w.at[0, 0, 0], local_sem.at[0]),
        pltpu.make_async_copy(up.at[pl.ds(half, half)], w.at[0, 0, 1], local_sem.at[8]),
        pltpu.make_async_copy(down.at[pl.ds(0, half)], w.at[1, 0, 0], local_sem.at[1]),
        pltpu.make_async_copy(down.at[pl.ds(half, half)], w.at[1, 0, 1], local_sem.at[2]),
        pltpu.make_async_copy(patches, pv, local_sem.at[3]),
        pltpu.make_async_copy(keys, kv, local_sem.at[4]),
        pltpu.make_async_copy(values, vv, local_sem.at[5]),
        pltpu.make_async_copy(ow, owv, local_sem.at[6]),
    ]
    for load in loads:
        load.start()

    row = lax.broadcasted_iota(jnp.int32, (8, 128), 0)
    lane = lax.broadcasted_iota(jnp.int32, (8, 128), 1)
    meta = jnp.zeros((8, 128), jnp.int32)
    for s in range(slots):
        meta = jnp.where((row == 0) & (lane == s), counts[s], meta)
        meta = jnp.where((row == 1) & (lane == s), enc[s], meta)
    meta_out[...] = meta
    meta_in[y] = meta

    pl.semaphore_wait(barrier, n_tp + n_dp - 1)

    def x_copy(k, d, r):
        rows = pl.ds(*lanes[k])
        return rcopy(
            w.at[:, r, d, rows],
            w.at[:, r + 1, d, rows],
            x_send,
            x_recv.at[k, d, r],
            tp=right if d == 0 else left,
        )

    def z_copy(d, r):
        at = w.at[:, r, d, pl.ds(zmine, zrows)]
        return rcopy(at, at, z_send, z_recv.at[d, r], group=peer)

    def y_copy(d, r):
        at = w.at[:, r, d, pl.ds(ymine, yrows)]
        return rcopy(at, at, y_send, y_recv.at[d, r], dp=above if d == 0 else below)

    for load in loads[:4]:
        load.wait()
    for k in (0, 1):
        for d in (0, 1):
            x_copy(k, d, 0).start()

    loads[4].wait()

    def stage(e, carry):
        slot = jnp.int32(0)
        for s in range(slots):
            slot = slot + jnp.where((counts[s] > 0) & (enc[s] == e), s, 0)
        outgoing[e] = pv[slot]
        return carry

    lax.fori_loop(0, n_dp, stage, 0)
    for d in range(1, n_dp):
        to = lax.rem(y + d, n_dp)
        rcopy(meta_out, meta_in.at[y], m_sem.at[0], m_sem.at[1], dp=to).start()
    far_first = sorted(range(1, n_dp), key=lambda d: -min(d, n_dp - d))
    for p in range(PARTS):
        for d in far_first:
            to = lax.rem(y + d, n_dp)
            rcopy(
                outgoing.at[to, pl.ds(p * few, few)],
                arrived[p].at[y],
                a_send,
                a_recv.at[p],
                dp=to,
            ).start()
    for p in range(PARTS):
        arrived[p][y] = outgoing[y, p * few : (p + 1) * few, :]

    seqs, kvh, span, hd = kv.shape
    per = q.shape[1] // kvh
    scale = hd**-0.5
    own_heads = (kvh * per) // n_tp

    def attend_local():
        loads[5].wait()
        loads[6].wait()
        wide = lax.broadcasted_iota(jnp.int32, (per, 128), 1)
        for s in range(seqs):
            pos = t * span + lax.broadcasted_iota(jnp.int32, (per, span), 1)
            valid = pos < lens[s]
            for h in range(kvh):
                query = q[s, h * per : (h + 1) * per, :]
                scores = (
                    lax.dot_general(
                        query, kv[s, h], (((1,), (1,)), ((), ())), preferred_element_type=F32
                    )
                    * scale
                )
                scores = jnp.where(valid, scores, -1e30)
                own = (
                    jnp.sum(
                        query.astype(F32) * nk[s, h : h + 1, :].astype(F32), axis=1, keepdims=True
                    )
                    * scale
                )
                top = jnp.maximum(jnp.max(scores, axis=1, keepdims=True), own)
                weights = jnp.exp(scores - top)
                total = jnp.sum(weights, axis=1, keepdims=True)
                mix = jnp.dot(weights.astype(BF16), vv[s, h], preferred_element_type=F32)
                stats = jnp.where(wide < 64, top, total)
                ownw = jnp.broadcast_to(own, (per, 128))
                fresh = nv[s, h : h + 1, :].astype(F32)
                for i in range(per):
                    head = h * per + i
                    p, j = head // own_heads, head % own_heads
                    at = seqs * j + s
                    rs_src[p, at : at + 1, :] = mix[i : i + 1, :]
                    rs_src[p, 8 + at : 9 + at, :] = stats[i : i + 1, :]
                    own_buf[p, at : at + 1, :] = ownw[i : i + 1, :]
                    nv_buf[p, at : at + 1, :] = fresh
        rs_dst[t] = rs_src[t]
        for d in range(1, n_tp):
            to = lax.rem(t + d, n_tp)
            rcopy(rs_src.at[to], rs_dst.at[t], rs_sem.at[0], rs_sem.at[1], tp=to).start()

    def attend_merge():
        some = pl.ds(0, n_tp - 1)
        drain(rs_dst.at[some], rs_sem.at[1])
        own = own_buf[t][:, 0:1]
        tops = [rs_dst[p, 8:16, 0:1] for p in range(n_tp)]
        top = own
        for m in tops:
            top = jnp.maximum(top, m)
        own_weight = jnp.exp(own - top)
        total = own_weight
        mixed = own_weight.astype(BF16).astype(F32) * nv_buf[t]
        for p in range(n_tp):
            factor = jnp.exp(tops[p] - top)
            total = total + rs_dst[p, 8:16, 64:65] * factor
            mixed = mixed + rs_dst[p, 0:8, :] * factor
        ag_dst[t] = (mixed / total).astype(BF16).astype(F32)
        for d in range(1, n_tp):
            to = lax.rem(t + d, n_tp)
            rcopy(ag_dst.at[t], ag_dst.at[t], ag_sem.at[0], ag_sem.at[1], tp=to).start()

    def project():
        loads[7].wait()
        drain(ag_dst.at[pl.ds(0, n_tp - 1)], ag_sem.at[1])
        wide = own_heads * hd
        total = jnp.zeros((8, owv.shape[1]), F32)
        which = lax.broadcasted_iota(jnp.int32, (8, hd), 0) // seqs
        for p in range(n_tp):
            block = ag_dst[p]
            lhs = jnp.concatenate(
                [jnp.where(which == j, block, 0.0) for j in range(own_heads)], axis=1
            ).astype(BF16)
            total = total + jnp.dot(
                lhs, owv[p * wide : (p + 1) * wide, :], preferred_element_type=F32
            )
        out = total[0:seqs]
        for j in range(1, own_heads):
            out = out + total[j * seqs : (j + 1) * seqs]
        dec[...] = out.astype(BF16)

    picked, kept = [], []
    both = CORES * RECV_MAX * few
    mine = RECV_MAX * few

    def plan():
        drain(meta_in.at[pl.ds(0, n_dp - 1)], m_sem.at[1])
        small = pltpu.make_async_copy(meta_in, meta_s, local_sem.at[7])
        small.start()
        small.wait()
        found = jnp.int32(0)
        pick = [jnp.int32(0)] * RECV_MAX
        keep = [jnp.int32(0)] * RECV_MAX
        for src in range(n_dp):
            count = jnp.int32(0)
            for s in range(slots):
                c = meta_s[src, 0, s]
                count = count + jnp.where((c > 0) & (meta_s[src, 1, s] == y), c, 0)
            for k in range(RECV_MAX):
                hit = (count > 0) & (found == k)
                pick[k] = jnp.where(hit, src, pick[k])
                keep[k] = jnp.where(hit, count, keep[k])
            found = found + jnp.where(count > 0, 1, 0)
        picked.extend(pick)
        kept.extend(keep)

    def tokens(p):
        here, there = pl.ds(0, mine), pl.ds(mine, mine)
        return rcopy(
            normed.at[p, here], normed.at[p, there], tok_send, tok_recv.at[p], tp=sib
        )

    def images(p):
        drain(arrived[p].at[pl.ds(0, n_dp - 1)], a_recv.at[p])
        for k in range(RECV_MAX):
            at = slice(k * few, (k + 1) * few)
            x = arrived[p][picked[k]].astype(F32)
            acc[p, at, :] = x
            center = x - jnp.mean(x, axis=1, keepdims=True)
            spread = jnp.mean(center * center, axis=1, keepdims=True)
            n = center * lax.rsqrt(spread + 1e-06) * gain[...].reshape(1, width)
            normed[p, at, :] = n.astype(BF16)
        tokens(p).start()
        acc[p, mine:both, :] = jnp.zeros((both - mine, width), F32)

    def turn(p):
        drain(normed.at[p, pl.ds(0, mine)], tok_recv.at[p])
        turned[p] = jnp.transpose(normed[p].astype(F32)).astype(BF16)

    def vit(r, count, p):
        units = count * w.shape[2] * half
        a = w[0, pl.ds(r, count)].reshape(units, width)
        b = w[1, pl.ds(r, count)].reshape(units, width)
        pre = jnp.dot(a, turned[p], preferred_element_type=F32)
        hidden = jnp.transpose(pre * jax.nn.sigmoid(1.702 * pre)).astype(BF16)
        acc[p] += jnp.dot(hidden, b, preferred_element_type=F32)

    def vit_range(lo, hi, p):
        count = 2 if (hi - lo) % 2 == 0 else 1

        def body(i, carry):
            vit(lo + i * count, count, p)
            return carry

        lax.fori_loop(0, (hi - lo) // count, body, 0)

    seen = set()

    def ready(r):
        if r == 0 or r in seen:
            return
        seen.add(r)
        for d in (0, 1):
            drain(w.at[:, r, d, pl.ds(zother, zrows)], z_recv.at[d, r])
            drain(w.at[:, r, d, pl.ds(yother, yrows)], y_recv.at[d, r])

    def compute(lo, hi, p):
        for r in range(lo, hi):
            ready(r)
        vit_range(lo, hi, p)

    def part(p):
        return rcopy(part_out.at[p], part_in.at[p], part_send, part_recv.at[p], tp=sib)

    def arrive(k, d, r):
        drain(w.at[:, r, d, pl.ds(*lanes[k])], x_recv.at[k, d, r - 1])
        if r < hops:
            x_copy(k, d, r).start()

    last = hops
    work = {
        1: [attend_local],
        2: [attend_merge],
        3: [project, plan],
        last - 3: [lambda: images(0)],
        last - 2: [lambda: turn(0), lambda: compute(0, last - 3, 0)],
        last - 1: [
            lambda: images(1),
            lambda: compute(last - 3, last - 1, 0),
            lambda: turn(1),
        ],
        last: [lambda: compute(0, last - 3, 1), lambda: compute(last - 3, last - 1, 1)],
    }
    for r in range(1, hops + 1):
        for d in (0, 1):
            arrive(0, d, r)
            z_copy(d, r).start()
        for d in (0, 1):
            arrive(1, d, r)
            y_copy(d, r).start()
        for d in (0, 1):
            if r == 1:
                x_copy(2, d, 0).start()
            else:
                arrive(2, d, r - 1)
        for task in work.get(r, ()):
            task()
    for p in range(PARTS):
        compute(last - 1, last, p)
    for d in (0, 1):
        arrive(2, d, hops)
    for p in range(PARTS):
        compute(last, last + 1, p)
        part_out[p] = acc[p, mine:both, :].astype(BF16)
        part(p).start()
    for p in range(PARTS):
        drain(part_in.at[p], part_recv.at[p])
        which = p * few + lax.broadcasted_iota(jnp.int32, (few, width), 0)
        for k in range(RECV_MAX):
            at = slice(k * few, (k + 1) * few)
            block = acc[p, at, :] + part_in[p, at, :].astype(F32)
            emb[k, p * few : (p + 1) * few, :] = jnp.where(which < kept[k], block, 0.0).astype(BF16)

    sent = zrows + yrows + drows
    drain(w.at[:, pl.ds(0, hops), :, pl.ds(0, sent)], x_send)
    drain(w.at[:, pl.ds(0, hops), :, pl.ds(0, zrows)], z_send)
    drain(w.at[:, pl.ds(0, hops), :, pl.ds(0, yrows)], y_send)
    drain(outgoing.at[pl.ds(0, n_dp - 1)], a_send)
    drain(meta_in.at[pl.ds(0, n_dp - 1)], m_sem.at[0])
    drain(rs_src.at[pl.ds(0, n_tp - 1)], rs_sem.at[0])
    drain(ag_dst.at[pl.ds(0, n_tp - 1)], ag_sem.at[0])
    drain(normed.at[:, pl.ds(0, mine)], tok_send)
    drain(part_out, part_send)


def local(sizes, *args):
    (
        patches,
        patch_counts,
        encoder_index,
        vit_gain,
        vit_up,
        vit_down,
        queries,
        cache_keys,
        cache_values,
        new_keys,
        new_values,
        kv_lengths,
        out_weight,
    ) = args
    n_tp, n_dp = sizes
    slots, rows, width = patches.shape
    units = vit_down.shape[0]
    half = units // 2
    ring = n_tp // CORES
    mine = RECV_MAX * rows // PARTS
    seqs = queries.shape[0]
    columns = out_weight.shape[1]
    smem = pl.BlockSpec(memory_space=pltpu.SMEM)
    vmem = pl.BlockSpec(memory_space=pltpu.VMEM)
    hbm = pl.BlockSpec(memory_space=pl.ANY)
    dma = pltpu.SemaphoreType.DMA
    return pl.pallas_call(
        functools.partial(kernel, sizes),
        out_shape=(
            jax.ShapeDtypeStruct((RECV_MAX, rows, width), BF16),
            jax.ShapeDtypeStruct((seqs, columns), BF16),
        ),
        in_specs=[smem, smem, smem, hbm, vmem, hbm, hbm, vmem, hbm, hbm, vmem, vmem, hbm],
        out_specs=(vmem, vmem),
        scratch_shapes=[
            pltpu.VMEM((2, ring, 2, half, width), BF16),
            pltpu.VMEM(patches.shape, BF16),
            pltpu.VMEM((n_dp, rows, width), BF16),
            pltpu.VMEM((n_dp, rows // PARTS, width), BF16),
            pltpu.VMEM((n_dp, rows // PARTS, width), BF16),
            pltpu.VMEM(cache_keys.shape, BF16),
            pltpu.VMEM(cache_values.shape, BF16),
            pltpu.VMEM(out_weight.shape, BF16),
            pltpu.VMEM((8, 128), jnp.int32),
            pltpu.VMEM((n_dp, 8, 128), jnp.int32),
            pltpu.SMEM((n_dp, 8, 128), jnp.int32),
            pltpu.VMEM((n_tp, 16, 128), F32),
            pltpu.VMEM((n_tp, 16, 128), F32),
            pltpu.VMEM((n_tp, 8, 128), F32),
            pltpu.VMEM((n_tp, 8, 128), F32),
            pltpu.VMEM((n_tp, 8, 128), F32),
            pltpu.VMEM((PARTS, CORES * mine, width), BF16),
            pltpu.VMEM((PARTS, width, CORES * mine), BF16),
            pltpu.VMEM((PARTS, CORES * mine, width), F32),
            pltpu.VMEM((PARTS, mine, width), BF16),
            pltpu.VMEM((PARTS, mine, width), BF16),
            dma((9,)),
            dma((3, 2, ring - 1)),
            dma((2, ring)),
            dma((2, ring)),
            dma,
            dma,
            dma,
            dma,
            dma((PARTS,)),
            dma((2,)),
            dma((2,)),
            dma((2,)),
            dma,
            dma((PARTS,)),
            dma,
            dma((PARTS,)),
        ],
        compiler_params=pltpu.CompilerParams(
            collective_id=0, has_side_effects=True, vmem_limit_bytes=62 * 1024 * 1024
        ),
        name="step",
    )(
        patch_counts,
        encoder_index,
        kv_lengths,
        patches,
        vit_gain,
        vit_up.T,
        vit_down,
        queries,
        cache_keys,
        cache_values,
        new_keys,
        new_values,
        out_weight,
    )


def solution(mesh):
    assert mesh.shape["group"] % 2 == 0 and mesh.shape["dp"] % 2 == 0
    sizes = (mesh.shape["tp"], mesh.shape["dp"])
    return jax.shard_map(
        functools.partial(local, sizes),
        mesh=mesh,
        in_specs=(
            P(("group", "tp", "dp"), None, None),
            P(("group", "tp", "dp")),
            P(("group", "tp", "dp")),
            P(),
            P(None, "tp"),
            P("tp", None),
            P(("group", "dp"), None, None),
            P(("group", "dp"), None, "tp", None),
            P(("group", "dp"), None, "tp", None),
            P(("group", "dp"), None, None),
            P(("group", "dp"), None, None),
            P(("group", "dp")),
            P(None, "tp"),
        ),
        out_specs=(P(("group", "tp", "dp"), None, None), P(("group", "dp"), "tp")),
        check_vma=False,
    )
```

```python
import functools

import jax
import jax.numpy as jnp
from jax import lax
from jax.experimental import pallas as pl
from jax.experimental.pallas import tpu as pltpu
from jax.sharding import PartitionSpec as P

MESH = pl.DeviceIdType.MESH
RECV_MAX = 3
CORES = 2
PARTS = 1
F32 = jnp.float32
BF16 = jnp.bfloat16


def rcopy(src, dst, send, recv, **where):
    return pltpu.make_async_remote_copy(
        src_ref=src,
        dst_ref=dst,
        send_sem=send,
        recv_sem=recv,
        device_id=where,
        device_id_type=MESH,
    )


def drain(ref, sem):
    pltpu.make_async_copy(ref, ref, sem).wait()


Z_PARTS = (6, 6)
Y_PARTS = (2, 2)


def kernel(
    sizes,
    counts,
    enc,
    lens,
    patches,
    gain,
    up,
    down,
    q,
    keys,
    values,
    nk,
    nv,
    ow,
    emb,
    dec,
    w,
    pv,
    outgoing,
    arrived_a,
    kv,
    vv,
    owv,
    meta_out,
    meta_in,
    meta_s,
    rs_src,
    rs_dst,
    ag_dst,
    own_buf,
    nv_buf,
    normed,
    turned,
    acc,
    part_out,
    part_in,
    local_sem,
    x_recv,
    z_recv,
    y_recv,
    x_send,
    z_send,
    y_send,
    a_send,
    a_recv,
    m_sem,
    rs_sem,
    ag_sem,
    tok_send,
    tok_recv,
    part_send,
    part_recv,
):
    n_tp, n_dp = sizes
    ring = n_tp // CORES
    hops = ring - 1
    half = w.shape[3]
    zrows = [n * half // 20 for n in Z_PARTS]
    yrows = [n * half // 20 for n in Y_PARTS]
    drows = [half - 2 * a - 2 * b for a, b in zip(zrows, yrows)]
    t = lax.axis_index("tp")
    y = lax.axis_index("dp")
    g = lax.axis_index("group")
    gpar = lax.rem(g, 2)
    ypar = lax.rem(y, 2)
    core = lax.rem(t, CORES)
    right = lax.rem(t + CORES, n_tp)
    left = lax.rem(t + n_tp - CORES, n_tp)
    sib = t + 1 - 2 * core
    peer = g + 1 - 2 * gpar
    above, below = lax.rem(y + 1, n_dp), lax.rem(y + n_dp - 1, n_dp)
    zmine, ymine, direct, zother, yother = [], [], [], [], []
    for zr, yr, dr in zip(zrows, yrows, drows):
        zmine.append(pl.ds(pl.multiple_of(gpar * (half - zr), 8), zr))
        zother.append(pl.ds(pl.multiple_of((1 - gpar) * (half - zr), 8), zr))
        ymine.append(pl.ds(pl.multiple_of(zr + ypar * (yr + dr), 8), yr))
        yother.append(pl.ds(pl.multiple_of(zr + (1 - ypar) * (yr + dr), 8), yr))
        direct.append(pl.ds(zr + yr, dr))
    lanes = (zmine, ymine, direct)
    slots, rows, width = patches.shape
    few = rows // PARTS
    arrived = (arrived_a,)

    barrier = pltpu.get_barrier_semaphore()
    for d in range(1, n_tp):
        pl.semaphore_signal(
            barrier, inc=1, device_id={"tp": lax.rem(t + d, n_tp)}, device_id_type=MESH
        )
    for d in range(1, n_dp):
        pl.semaphore_signal(
            barrier, inc=1, device_id={"dp": lax.rem(y + d, n_dp)}, device_id_type=MESH
        )
    pl.semaphore_signal(barrier, inc=1, device_id={"group": peer}, device_id_type=MESH)

    loads = [
        pltpu.make_async_copy(up.at[pl.ds(0, half)], w.at[0, 0, 0], local_sem.at[0]),
        pltpu.make_async_copy(up.at[pl.ds(half, half)], w.at[0, 0, 1], local_sem.at[8]),
        pltpu.make_async_copy(down.at[pl.ds(0, half)], w.at[1, 0, 0], local_sem.at[1]),
        pltpu.make_async_copy(down.at[pl.ds(half, half)], w.at[1, 0, 1], local_sem.at[2]),
        pltpu.make_async_copy(patches, pv, local_sem.at[3]),
        pltpu.make_async_copy(keys, kv, local_sem.at[4]),
        pltpu.make_async_copy(values, vv, local_sem.at[5]),
        pltpu.make_async_copy(ow, owv, local_sem.at[6]),
    ]
    for load in loads:
        load.start()

    row = lax.broadcasted_iota(jnp.int32, (8, 128), 0)
    lane = lax.broadcasted_iota(jnp.int32, (8, 128), 1)
    meta = jnp.zeros((8, 128), jnp.int32)
    for s in range(slots):
        meta = jnp.where((row == 0) & (lane == s), counts[s], meta)
        meta = jnp.where((row == 1) & (lane == s), enc[s], meta)
    meta_out[...] = meta
    meta_in[y] = meta

    pl.semaphore_wait(barrier, n_tp + n_dp - 1)

    def x_copy(k, d, r):
        rows = lanes[k][d]
        return rcopy(
            w.at[:, r, d, rows],
            w.at[:, r + 1, d, rows],
            x_send,
            x_recv.at[k, d, r],
            tp=right if d == 0 else left,
        )

    def z_copy(d, r):
        at = w.at[:, r, d, zmine[d]]
        return rcopy(at, at, z_send, z_recv.at[d, r], group=peer)

    def y_copy(d, r):
        at = w.at[:, r, d, ymine[d]]
        return rcopy(at, at, y_send, y_recv.at[d, r], dp=above if (d + r) % 2 else below)

    for load in loads[:4]:
        load.wait()
    for k in (0, 1):
        for d in (0, 1):
            x_copy(k, d, 0).start()

    loads[4].wait()

    def stage(e, carry):
        slot = jnp.int32(0)
        for s in range(slots):
            slot = slot + jnp.where((counts[s] > 0) & (enc[s] == e), s, 0)
        outgoing[e] = pv[slot]
        return carry

    lax.fori_loop(0, n_dp, stage, 0)
    far_first = sorted(range(1, n_dp), key=lambda d: -min(d, n_dp - d))

    for i, d in enumerate(far_first):
        to = lax.rem(y + d, n_dp)
        rcopy(outgoing.at[to], arrived[0].at[y], a_send, a_recv.at[0], dp=to).start()
        if i == 2:
            for e in far_first:
                to = lax.rem(y + e, n_dp)
                rcopy(meta_out, meta_in.at[y], m_sem.at[0], m_sem.at[1], dp=to).start()
    for p in range(PARTS):
        arrived[p][y] = outgoing[y, p * few : (p + 1) * few, :]

    seqs, kvh, span, hd = kv.shape
    per = q.shape[1] // kvh
    scale = hd**-0.5
    own_heads = (kvh * per) // n_tp

    def attend_local():
        loads[5].wait()
        loads[6].wait()
        wide = lax.broadcasted_iota(jnp.int32, (per, 128), 1)
        for s in range(seqs):
            pos = t * span + lax.broadcasted_iota(jnp.int32, (per, span), 1)
            valid = pos < lens[s]
            for h in range(kvh):
                query = q[s, h * per : (h + 1) * per, :]
                scores = (
                    lax.dot_general(
                        query, kv[s, h], (((1,), (1,)), ((), ())), preferred_element_type=F32
                    )
                    * scale
                )
                scores = jnp.where(valid, scores, -1e30)
                own = (
                    jnp.sum(
                        query.astype(F32) * nk[s, h : h + 1, :].astype(F32), axis=1, keepdims=True
                    )
                    * scale
                )
                top = jnp.maximum(jnp.max(scores, axis=1, keepdims=True), own)
                weights = jnp.exp(scores - top)
                total = jnp.sum(weights, axis=1, keepdims=True)
                mix = jnp.dot(weights.astype(BF16), vv[s, h], preferred_element_type=F32)
                stats = jnp.where(wide < 64, top, total)
                ownw = jnp.broadcast_to(own, (per, 128))
                fresh = nv[s, h : h + 1, :].astype(F32)
                for i in range(per):
                    head = h * per + i
                    p, j = head // own_heads, head % own_heads
                    at = seqs * j + s
                    rs_src[p, at : at + 1, :] = mix[i : i + 1, :]
                    rs_src[p, 8 + at : 9 + at, :] = stats[i : i + 1, :]
                    own_buf[p, at : at + 1, :] = ownw[i : i + 1, :]
                    nv_buf[p, at : at + 1, :] = fresh
        rs_dst[t] = rs_src[t]
        for d in range(1, n_tp):
            to = lax.rem(t + d, n_tp)
            rcopy(rs_src.at[to], rs_dst.at[t], rs_sem.at[0], rs_sem.at[1], tp=to).start()

    def attend_merge():
        some = pl.ds(0, n_tp - 1)
        drain(rs_dst.at[some], rs_sem.at[1])
        own = own_buf[t][:, 0:1]
        tops = [rs_dst[p, 8:16, 0:1] for p in range(n_tp)]
        top = own
        for m in tops:
            top = jnp.maximum(top, m)
        own_weight = jnp.exp(own - top)
        total = own_weight
        mixed = own_weight.astype(BF16).astype(F32) * nv_buf[t]
        for p in range(n_tp):
            factor = jnp.exp(tops[p] - top)
            total = total + rs_dst[p, 8:16, 64:65] * factor
            mixed = mixed + rs_dst[p, 0:8, :] * factor
        ag_dst[t] = (mixed / total).astype(BF16).astype(F32)
        for d in range(1, n_tp):
            to = lax.rem(t + d, n_tp)
            rcopy(ag_dst.at[t], ag_dst.at[t], ag_sem.at[0], ag_sem.at[1], tp=to).start()

    def project():
        loads[7].wait()
        drain(ag_dst.at[pl.ds(0, n_tp - 1)], ag_sem.at[1])
        wide = own_heads * hd
        total = jnp.zeros((8, owv.shape[1]), F32)
        which = lax.broadcasted_iota(jnp.int32, (8, hd), 0) // seqs
        for p in range(n_tp):
            block = ag_dst[p]
            lhs = jnp.concatenate(
                [jnp.where(which == j, block, 0.0) for j in range(own_heads)], axis=1
            ).astype(BF16)
            total = total + jnp.dot(
                lhs, owv[p * wide : (p + 1) * wide, :], preferred_element_type=F32
            )
        out = total[0:seqs]
        for j in range(1, own_heads):
            out = out + total[j * seqs : (j + 1) * seqs]
        dec[...] = out.astype(BF16)

    picked, kept = [], []
    both = CORES * RECV_MAX * few
    mine = RECV_MAX * few

    def plan():
        drain(meta_in.at[pl.ds(0, n_dp - 1)], m_sem.at[1])
        small = pltpu.make_async_copy(meta_in, meta_s, local_sem.at[7])
        small.start()
        small.wait()
        found = jnp.int32(0)
        pick = [jnp.int32(0)] * RECV_MAX
        keep = [jnp.int32(0)] * RECV_MAX
        for src in range(n_dp):
            count = jnp.int32(0)
            for s in range(slots):
                c = meta_s[src, 0, s]
                count = count + jnp.where((c > 0) & (meta_s[src, 1, s] == y), c, 0)
            for k in range(RECV_MAX):
                hit = (count > 0) & (found == k)
                pick[k] = jnp.where(hit, src, pick[k])
                keep[k] = jnp.where(hit, count, keep[k])
            found = found + jnp.where(count > 0, 1, 0)
        picked.extend(pick)
        kept.extend(keep)

    def tokens(p):
        here, there = pl.ds(0, mine), pl.ds(mine, mine)
        return rcopy(
            normed.at[p, here], normed.at[p, there], tok_send, tok_recv.at[p], tp=sib
        )

    def images(p):
        drain(arrived[p].at[pl.ds(0, n_dp - 1)], a_recv.at[p])
        for k in range(RECV_MAX):
            at = slice(k * few, (k + 1) * few)
            x = arrived[p][picked[k]].astype(F32)
            acc[p, at, :] = x
            center = x - jnp.mean(x, axis=1, keepdims=True)
            spread = jnp.mean(center * center, axis=1, keepdims=True)
            n = center * lax.rsqrt(spread + 1e-06) * gain[...].reshape(1, width)
            normed[p, at, :] = n.astype(BF16)
        tokens(p).start()
        acc[p, mine:both, :] = jnp.zeros((both - mine, width), F32)

    def turn(p):
        drain(normed.at[p, pl.ds(0, mine)], tok_recv.at[p])
        turned[p] = jnp.transpose(normed[p].astype(F32)).astype(BF16)

    def vit(r, count, p):
        units = count * w.shape[2] * half
        a = w[0, pl.ds(r, count)].reshape(units, width)
        b = w[1, pl.ds(r, count)].reshape(units, width)
        pre = jnp.dot(a, turned[p], preferred_element_type=F32)
        hidden = (pre * jax.nn.sigmoid(1.702 * pre)).astype(BF16)
        acc[p] += lax.dot_general(hidden, b, (((0,), (0,)), ((), ())), preferred_element_type=F32)

    def vit_range(lo, hi, p):
        count = 2 if (hi - lo) % 2 == 0 else 1

        def body(i, carry):
            vit(lo + i * count, count, p)
            return carry

        lax.fori_loop(0, (hi - lo) // count, body, 0)

    seen = set()

    def ready(r):
        if r == 0 or r in seen:
            return
        seen.add(r)
        for d in (0, 1):
            drain(w.at[:, r, d, zother[d]], z_recv.at[d, r])
            drain(w.at[:, r, d, yother[d]], y_recv.at[d, r])

    def compute(lo, hi, p):
        for r in range(lo, hi):
            ready(r)
        vit_range(lo, hi, p)

    def part(p):
        return rcopy(part_out.at[p], part_in.at[p], part_send, part_recv.at[p], tp=sib)

    def arrive(k, d, r):
        drain(w.at[:, r, d, lanes[k][d]], x_recv.at[k, d, r - 1])
        if r < hops:
            x_copy(k, d, r).start()

    last = hops
    work = {
        1: [attend_local],
        2: [attend_merge],
        3: [project],
        4: [plan],
        last - 2: [lambda: images(0)],
        last - 1: [lambda: turn(0), lambda: compute(0, last - 3, 0)],
        last: [lambda: compute(last - 3, last - 1, 0)],
    }
    for r in range(1, hops + 1):
        for d in (0, 1):
            arrive(0, d, r)
            z_copy(d, r).start()
        for d in (0, 1):
            arrive(1, d, r)
            y_copy(d, r).start()
        for d in (0, 1):
            if r == 1:
                x_copy(2, d, 0).start()
            else:
                arrive(2, d, r - 1)
        for task in work.get(r, ()):
            task()
    for p in range(PARTS):
        compute(last - 1, last, p)
    for d in (0, 1):
        arrive(2, d, hops)
    for p in range(PARTS):
        compute(last, last + 1, p)
        part_out[p] = acc[p, mine:both, :].astype(BF16)
        part(p).start()
    for p in range(PARTS):
        drain(part_in.at[p], part_recv.at[p])
        which = p * few + lax.broadcasted_iota(jnp.int32, (few, width), 0)
        for k in range(RECV_MAX):
            at = slice(k * few, (k + 1) * few)
            block = acc[p, at, :] + part_in[p, at, :].astype(F32)
            emb[k, p * few : (p + 1) * few, :] = jnp.where(which < kept[k], block, 0.0).astype(BF16)

    sent = sum(zrows) + sum(yrows) + sum(drows)
    for sem, size in ((x_send, sent), (z_send, sum(zrows)), (y_send, sum(yrows))):
        drain(w.at[:, pl.ds(0, hops), 0, pl.ds(0, size)] if size <= half else w.at[:, pl.ds(0, hops), :, pl.ds(0, size // 2)], sem)
    drain(outgoing.at[pl.ds(0, n_dp - 1)], a_send)
    drain(meta_in.at[pl.ds(0, n_dp - 1)], m_sem.at[0])
    drain(rs_src.at[pl.ds(0, n_tp - 1)], rs_sem.at[0])
    drain(ag_dst.at[pl.ds(0, n_tp - 1)], ag_sem.at[0])
    drain(normed.at[:, pl.ds(0, mine)], tok_send)
    drain(part_out, part_send)


def local(sizes, *args):
    (
        patches,
        patch_counts,
        encoder_index,
        vit_gain,
        vit_up,
        vit_down,
        queries,
        cache_keys,
        cache_values,
        new_keys,
        new_values,
        kv_lengths,
        out_weight,
    ) = args
    n_tp, n_dp = sizes
    slots, rows, width = patches.shape
    units = vit_down.shape[0]
    half = units // 2
    ring = n_tp // CORES
    mine = RECV_MAX * rows // PARTS
    seqs = queries.shape[0]
    columns = out_weight.shape[1]
    smem = pl.BlockSpec(memory_space=pltpu.SMEM)
    vmem = pl.BlockSpec(memory_space=pltpu.VMEM)
    hbm = pl.BlockSpec(memory_space=pl.ANY)
    dma = pltpu.SemaphoreType.DMA
    emb, dec = pl.pallas_call(
        functools.partial(kernel, sizes),
        out_shape=(
            jax.ShapeDtypeStruct((RECV_MAX, rows, width), BF16),
            jax.ShapeDtypeStruct((seqs, columns), BF16),
        ),
        in_specs=[smem, smem, smem, hbm, vmem, hbm, hbm, vmem, hbm, hbm, vmem, vmem, hbm],
        out_specs=(vmem, vmem),
        scratch_shapes=[
            pltpu.VMEM((2, ring, 2, half, width), BF16),
            pltpu.VMEM(patches.shape, BF16),
            pltpu.VMEM((n_dp, rows, width), BF16),
            pltpu.VMEM((n_dp, rows // PARTS, width), BF16),
            pltpu.VMEM(cache_keys.shape, BF16),
            pltpu.VMEM(cache_values.shape, BF16),
            pltpu.VMEM(out_weight.shape, BF16),
            pltpu.VMEM((8, 128), jnp.int32),
            pltpu.VMEM((n_dp, 8, 128), jnp.int32),
            pltpu.SMEM((n_dp, 8, 128), jnp.int32),
            pltpu.VMEM((n_tp, 16, 128), F32),
            pltpu.VMEM((n_tp, 16, 128), F32),
            pltpu.VMEM((n_tp, 8, 128), F32),
            pltpu.VMEM((n_tp, 8, 128), F32),
            pltpu.VMEM((n_tp, 8, 128), F32),
            pltpu.VMEM((PARTS, CORES * mine, width), BF16),
            pltpu.VMEM((PARTS, width, CORES * mine), BF16),
            pltpu.VMEM((PARTS, CORES * mine, width), F32),
            pltpu.VMEM((PARTS, mine, width), BF16),
            pltpu.VMEM((PARTS, mine, width), BF16),
            dma((9,)),
            dma((3, 2, ring - 1)),
            dma((2, ring)),
            dma((2, ring)),
            dma,
            dma,
            dma,
            dma,
            dma((PARTS,)),
            dma((2,)),
            dma((2,)),
            dma((2,)),
            dma,
            dma((PARTS,)),
            dma,
            dma((PARTS,)),
        ],
        compiler_params=pltpu.CompilerParams(
            collective_id=0, has_side_effects=True, vmem_limit_bytes=62 * 1024 * 1024
        ),
        name="step",
    )(
        patch_counts,
        encoder_index,
        kv_lengths,
        patches,
        vit_gain,
        vit_up.T,
        vit_down,
        queries,
        cache_keys,
        cache_values,
        new_keys,
        new_values,
        out_weight,
    )
    return pl.pallas_call(
        close,
        out_shape=(
            jax.ShapeDtypeStruct(emb.shape, BF16),
            jax.ShapeDtypeStruct(dec.shape, BF16),
        ),
        in_specs=[vmem, vmem],
        out_specs=(vmem, vmem),
        name="close",
    )(emb, dec)


def close(emb, dec, emb_out, dec_out):
    emb_out[...] = emb[...]
    dec_out[...] = dec[...]


def solution(mesh):
    assert mesh.shape["group"] % 2 == 0 and mesh.shape["dp"] % 2 == 0
    sizes = (mesh.shape["tp"], mesh.shape["dp"])
    return jax.shard_map(
        functools.partial(local, sizes),
        mesh=mesh,
        in_specs=(
            P(("group", "tp", "dp"), None, None),
            P(("group", "tp", "dp")),
            P(("group", "tp", "dp")),
            P(),
            P(None, "tp"),
            P("tp", None),
            P(("group", "dp"), None, None),
            P(("group", "dp"), None, "tp", None),
            P(("group", "dp"), None, "tp", None),
            P(("group", "dp"), None, None),
            P(("group", "dp"), None, None),
            P(("group", "dp")),
            P(None, "tp"),
        ),
        out_specs=(P(("group", "tp", "dp"), None, None), P(("group", "dp"), "tp")),
        check_vma=False,
    )
```
